128 devices in a mesh: level: 4 (over x_lo, core), space: 32 (over y, x_hi, z).
Axes of the slice: x: 4 (x_hi: 2, x_lo: 2; x = x_hi * 2 + x_lo), y: 4, z: 4, core: 2. Of those that a mesh axis runs over, the one named last changes fastest.
Arguments:
- u_init: float32 [1024, 2048], P('space'), may hold values from 0.2 to 1
- v_init: float32 [1024, 2048], P('space'), may hold values from 0 to 0.5
- feed_rate: float32 [1024, 2048], P('space'), may hold values from 0.01 to 0.12
- kill_rate: float32 [1024, 2048], P('space'), may hold values from 0.02 to 0.16
Outputs:
- level_states: float32 [4, 2, 1024, 2048], P('level', None, 'space')
The draws below stay inside these ranges and needn't reach their ends.
All inputs are finite; a program needn't handle non-finite values.
Results may differ from the reference program's by a relative error of at most 0.0003.
Values sent between devices are 32-bit elements; how exact they have to be, the bound alone decides.
A program may use at most 64 MiB of HBM per device.

```python
import math
import jax
import jax.numpy as jnp
from jax import lax

NX = 2048
STEPS = 4
SWEEPS = 3
NY = 1024
N_LEVEL = 4


def block_levels(stream_key, shape, cuts, least, top_value):
    gain = 1.0
    for axis_at, shards_of in cuts:
        draws = jax.random.uniform(jax.random.fold_in(jax.random.fold_in(stream_key, 6), axis_at), (shards_of,), jnp.float32, least / len(cuts), top_value / len(cuts))
        gain = gain * jnp.repeat(jnp.exp(draws), shape[axis_at] // shards_of).reshape((-1,) + (1,) * (len(shape) - 1 - axis_at))
    return gain


def setup_inputs(seed: int = 0) -> dict:
    splits = jax.random.split(jax.random.key(seed), 5)
    return {
        "u_init": jnp.clip(0.2 + 0.8 * jax.random.uniform(splits[0], (NY, NX), jnp.float32) ** block_levels(splits[0], (NY, NX), ((0, 32),), -0.2, 0.2), 0.2, 1.0),
        "v_init": jnp.clip(0.5 * jax.random.uniform(splits[1], (NY, NX), jnp.float32) ** block_levels(splits[1], (NY, NX), ((0, 32),), -0.2, 0.2), 0.0, 0.5),
        "feed_rate": jnp.clip(jnp.exp(math.log(0.12) - 2.4849066 * jax.random.uniform(splits[2], (NY, NX), jnp.float32) ** block_levels(splits[2], (NY, NX), ((0, 32),), -0.2, 0.2)), 0.01, 0.12),
        "kill_rate": jnp.clip(jnp.exp(math.log(0.16) - 2.0794415 * jax.random.uniform(splits[3], (NY, NX), jnp.float32) ** block_levels(splits[3], (NY, NX), ((0, 32),), -0.2, 0.2)), 0.02, 0.16),
    }


time_step = 1.0
diffusion = (1.0, 0.5)
quad_weights = [[9.0, 19.0, -5.0, 1.0, 0.0], [-1.0, 13.0, 13.0, -1.0, 0.0], [1.0, -5.0, 19.0, 9.0, 0.0], [0.0, 1.0, -5.0, 19.0, 9.0]]


def diffusion_rates():
    return jnp.array(diffusion, jnp.float32)[:, None, None]


def reaction(state, feed_rate, kill_rate):
    u_field = state[0]
    v_field = state[1]
    uv_square = u_field * v_field * v_field
    return jnp.stack([-uv_square + feed_rate * (1.0 - u_field), uv_square - (feed_rate + kill_rate) * v_field])


def neighbours(iterate):
    return jnp.roll(iterate, 1, 1) + jnp.roll(iterate, -1, 1) + jnp.roll(iterate, 1, 2) + jnp.roll(iterate, -1, 2)


def laplace(state):
    return diffusion_rates() * (neighbours(state) - 4.0 * state)


def jacobi_solve(source):
    step_rate = time_step * diffusion_rates()
    iterate = source
    for sweep_idx in range(SWEEPS):
        iterate = (source + step_rate * neighbours(iterate)) / (1.0 + 4.0 * step_rate)
    return iterate


def reference(u_init, v_init, feed_rate, kill_rate):
    weight_table = jnp.array(quad_weights, jnp.float32) / 24.0
    initial = jnp.stack([u_init, v_init])
    prev_lap = None
    prev_rea = None
    final_list = []
    for level_idx in range(N_LEVEL):
        state = initial
        node_list = [initial]
        for step_idx in range(STEPS):
            source = state + time_step * reaction(state, feed_rate, kill_rate)
            if level_idx > 0:
                forcing = prev_lap + prev_rea
                quadrature = time_step * jnp.einsum("m,mfij->fij", weight_table[step_idx], forcing, precision=lax.Precision.HIGHEST)
                source = source + (quadrature - time_step * prev_lap[step_idx + 1] - time_step * prev_rea[step_idx])
            state = jacobi_solve(source)
            node_list.append(state)
        final_list.append(state)
        prev_lap = jnp.stack([laplace(node_value) for node_value in node_list])
        prev_rea = jnp.stack([reaction(node_value, feed_rate, kill_rate) for node_value in node_list])
    return jnp.stack(final_list)
```

```python
import jax
import jax.numpy as jnp
from jax import lax
from jax.experimental import pallas as pl
from jax.experimental.pallas import tpu as pltpu
from jax.sharding import PartitionSpec as P

STEPS = 4
LEVELS = 4
LANES = 128
TILES = 4
RING = TILES + 1
OFF = 56
MESH = pl.DeviceIdType.MESH

SOURCE_RADIUS = [[42, 39, 36, 15], [32, 29, 26, 11], [22, 19, 16, 7], [12, 9, 6, 3]]


def span(own, radius):
    low = (OFF - radius) // 8 * 8
    high = -(-(OFF + own + radius) // 8) * 8
    return low, high


def over_rows(low, high, chunk, body):
    count = (high - low) // chunk

    def step(i, carry):
        body(low + i * chunk, chunk)
        return carry

    if count:
        lax.fori_loop(0, count, step, 0, unroll=True)
    if low + count * chunk < high:
        body(low + count * chunk, high - low - count * chunk)


def around(ref, row, rows):
    mid = ref[:, pl.ds(row, rows), :]
    lane = lax.broadcasted_iota(jnp.int32, (1, rows, LANES), 2)
    to_right = pltpu.roll(mid, 1, 2)
    to_left = pltpu.roll(mid, LANES - 1, 2)
    left = jnp.where(lane == 0, jnp.concatenate([to_right[-1:], to_right[:-1]], 0), to_right)
    right = jnp.where(
        lane == LANES - 1, jnp.concatenate([to_left[1:], to_left[:1]], 0), to_left
    )
    return mid, (left + right) + (ref[:, pl.ds(row - 1, rows), :] + ref[:, pl.ds(row + 1, rows), :])


def kernel(own, u_hbm, v_hbm, f_hbm, k_hbm, out, inp, side, node, force, first, work, fin,
           load_sem, side_sem, send_sem, recv_sem, put_sem, got_sem):
    level = lax.axis_index("level")
    space = lax.axis_index("space")
    blocks = lax.axis_size("space")
    cols = TILES * LANES
    near = [lax.rem(space + step, blocks) for step in (1, 2, blocks - 1, blocks - 2)]

    barrier = pltpu.get_barrier_semaphore()
    for peer in near:
        pl.semaphore_signal(barrier, inc=1, device_id={"space": peer}, device_id_type=MESH)
    for step in range(1, LEVELS):
        pl.semaphore_signal(
            barrier, inc=1, device_id={"level": lax.rem(level + step, LEVELS)}, device_id_type=MESH
        )

    left_col = pl.multiple_of(lax.rem(level + LEVELS - 1, LEVELS) * cols + cols - LANES, LANES)
    right_col = pl.multiple_of(lax.rem(level + 1, LEVELS) * cols, LANES)
    home = pl.ds(OFF, own)
    loads = []
    sides = []
    for at, field in enumerate((u_hbm, v_hbm, f_hbm, k_hbm)):
        for tile in range(TILES):
            col = pl.multiple_of(level * cols + tile * LANES, LANES)
            loads.append(pltpu.make_async_copy(
                field.at[:, pl.ds(col, LANES)], inp.at[at, tile, home, :], load_sem.at[at, tile]))
        for end, col in enumerate((left_col, right_col)):
            sides.append(pltpu.make_async_copy(
                field.at[:, pl.ds(col, LANES)], side.at[at, end], side_sem.at[at, end]))
    for copy in loads + sides:
        copy.start()
    for copy in sides:
        copy.wait()
    half = lax.broadcasted_iota(jnp.int32, (4, own, LANES), 2) < LANES // 2
    inp[:, TILES, home, :] = jnp.where(half, side[:, 1], side[:, 0])
    for copy in loads:
        copy.wait()
    pl.semaphore_wait(barrier, len(near) + LEVELS - 1)

    moves = [
        (OFF, OFF - own, own, near[0]),
        (OFF, OFF + own, own, near[2]),
        (OFF + own - 16, OFF - own - 16, 16, near[1]),
        (OFF, OFF + 2 * own, 16, near[3]),
    ]
    sends = []
    for part, tiles in enumerate((pl.ds(0, TILES), pl.ds(TILES, 1))):
        for at, (row, row_there, rows, peer) in enumerate(moves):
            sends.append(pltpu.make_async_remote_copy(
                inp.at[:, tiles, pl.ds(row, rows), :],
                inp.at[:, tiles, pl.ds(row_there, rows), :],
                send_sem.at[part, at], recv_sem.at[part, at],
                device_id={"space": peer}, device_id_type=MESH))
    for copy in sends:
        copy.start()
    for copy in sends:
        copy.wait()

    def rates(row, rows):
        here = pl.ds(row, rows)
        feed = inp[2, :, here, :]
        return feed, feed + inp[3, :, here, :]

    def react(u, v, feed, both):
        cubic = u * v * v
        return feed * (1.0 - u) - cubic, cubic - both * v

    def lap_of(ref, row, rows):
        mid, near_sum = around(ref, row, rows)
        return mid, near_sum - 4.0 * mid

    def first_forcing(row, rows):
        here = pl.ds(row, rows)
        feed, both = rates(row, rows)
        u, lap_u = lap_of(inp.at[0], row, rows)
        v, lap_v = lap_of(inp.at[1], row, rows)
        rea = react(u, v, feed, both)
        for field, total in enumerate((lap_u + rea[0], 0.5 * lap_v + rea[1])):
            first[0, field, :, here, :] = (9.0 / 24.0) * total - rea[field]
            first[1, field, :, here, :] = (1.0 / 24.0) * total

    def forcing(last, row, rows):
        here = pl.ds(row, rows)
        feed, both = rates(row, rows)
        count = STEPS if last else STEPS - 1
        laps = []
        reas = []
        for at in range(count):
            u, lap_u = lap_of(node.at[at, 0], row, rows)
            v, lap_v = lap_of(node.at[at, 1], row, rows)
            laps.append((lap_u, 0.5 * lap_v))
            if at < STEPS - 1 or last:
                reas.append(react(u, v, feed, both))
        for field in range(2):
            lap = [None] + [value[field] for value in laps]
            rea = [None] + [value[field] for value in reas]
            full = [None] + [a + b for a, b in zip(lap[1:], rea[1:])]
            nine = first[0, field, :, here, :]
            one = first[1, field, :, here, :]
            third = (1.0 / 24.0) * full[3]
            second = (5.0 / 24.0) * full[2]
            force[0, field, :, here, :] = (nine - lap[1]) + (19.0 / 24.0) * full[1] - second + third
            force[1, field, :, here, :] = (
                (13.0 / 24.0) * (full[1] + full[2]) - (one + third) - (lap[2] + rea[1]))
            force[2, field, :, here, :] = (
                (one - (lap[3] + rea[2])) - (5.0 / 24.0) * full[1]
                + (19.0 / 24.0) * full[2] + (9.0 / 24.0) * full[3])
            if last:
                force[3, field, :, here, :] = (
                    (1.0 / 24.0) * full[1] - second + (19.0 / 24.0) * full[3]
                    + (9.0 / 24.0) * full[4] - (lap[4] + rea[3]))

    def source(level_num, step_num, u_ref, v_ref, row, rows):
        here = pl.ds(row, rows)
        feed, both = rates(row, rows)
        u = u_ref[:, here, :]
        v = v_ref[:, here, :]
        rea_u, rea_v = react(u, v, feed, both)
        u = u + rea_u
        v = v + rea_v
        if level_num:
            u = u + force[step_num, 0, :, here, :]
            v = v + force[step_num, 1, :, here, :]
        work[0, 0, :, here, :] = 0.2 * u
        work[0, 1, :, here, :] = (1.0 / 3.0) * v

    def sweep(old, new, scale, field, row, rows):
        here = pl.ds(row, rows)
        _, near_sum = around(old, row, rows)
        if scale != 1.0:
            near_sum = scale * near_sum
        new[:, here, :] = work[0, field, :, here, :] + near_sum

    def last_sweep(old, scale, dest, field, row, rows):
        _, near_sum = around(old, row, rows)
        value = work[0, field, :, pl.ds(row, rows), :] + scale * near_sum
        for tile in range(TILES):
            dest[field, pl.ds(row - OFF, rows), pl.ds(tile * LANES, LANES)] = value[tile]

    puts = []
    for level_num in range(LEVELS):
        radii = SOURCE_RADIUS[level_num]
        if level_num == 1:
            over_rows(*span(own, radii[0]), 8, first_forcing)
        if level_num:
            low, high = span(own, radii[0])
            low_in, high_in = span(own, radii[3])
            over_rows(low, low_in, 8, lambda row, rows: forcing(False, row, rows))
            over_rows(low_in, high_in, 8, lambda row, rows: forcing(True, row, rows))
            over_rows(high_in, high, 8, lambda row, rows: forcing(False, row, rows))
        for step_num in range(STEPS):
            refs = [inp.at[field] if step_num == 0 else node.at[step_num - 1, field] for field in range(2)]
            radius = radii[step_num]
            over_rows(*span(own, radius), 16,
                      lambda row, rows: source(level_num, step_num, refs[0], refs[1], row, rows))
            for sweep_num in range(3):
                extent = span(own, radius - sweep_num - 1)
                for field, scale in enumerate((0.2, 1.0 / 6.0)):
                    old = work.at[sweep_num, field]
                    new = node.at[step_num, field] if sweep_num == 2 else work.at[sweep_num + 1, field]
                    factor = scale if sweep_num else (1.0, 0.5)[field]
                    if level_num == LEVELS - 1 and step_num == STEPS - 1 and sweep_num == 2:
                        over_rows(OFF, OFF + own, 16, lambda row, rows: last_sweep(
                            old, factor, fin.at[level_num], field, row, rows))
                    else:
                        over_rows(*extent, 16, lambda row, rows: sweep(
                            old, new, factor, field, row, rows))
        if level_num < LEVELS - 1:
            for field in range(2):
                for tile in range(TILES):
                    fin[level_num, field, :, pl.ds(tile * LANES, LANES)] = (
                        node[STEPS - 1, field, tile, home, :])
        place = out.at[0, :, :, pl.ds(pl.multiple_of(level * cols, LANES), cols)]
        mine = pltpu.make_async_copy(fin.at[level_num], place, put_sem.at[level_num])
        theirs = pltpu.make_async_remote_copy(
            fin.at[level_num], place, put_sem.at[level_num], got_sem.at[level],
            device_id={"level": level_num}, device_id_type=MESH)
        puts.append((mine, theirs))

        @pl.when(level == level_num)
        def _():
            mine.start()

        @pl.when(level != level_num)
        def _():
            theirs.start()

    for level_num, (mine, theirs) in enumerate(puts):
        @pl.when(level == level_num)
        def _():
            mine.wait()

        @pl.when(level != level_num)
        def _():
            theirs.wait_send()

    for step in range(1, LEVELS):
        source_level = lax.rem(level + step, LEVELS)
        place = out.at[0, :, :, pl.ds(pl.multiple_of(source_level * cols, LANES), cols)]
        pltpu.make_async_remote_copy(
            fin.at[0], place, put_sem.at[0], got_sem.at[source_level],
            device_id={"level": source_level}, device_id_type=MESH).wait_recv()


def body(u_init, v_init, feed_rate, kill_rate):
    own, width = u_init.shape
    rows = OFF + own + 56
    field = (RING, rows, LANES)
    anywhere = pl.BlockSpec(memory_space=pl.ANY)
    dma = pltpu.SemaphoreType.DMA
    return pl.pallas_call(
        lambda *refs: kernel(own, *refs),
        out_shape=jax.ShapeDtypeStruct((1, 2, own, width), jnp.float32),
        in_specs=[anywhere] * 4,
        out_specs=anywhere,
        scratch_shapes=[
            pltpu.VMEM((4,) + field, jnp.float32),
            pltpu.VMEM((4, 2, own, LANES), jnp.float32),
            pltpu.VMEM((STEPS, 2) + field, jnp.float32),
            pltpu.VMEM((STEPS, 2) + field, jnp.float32),
            pltpu.VMEM((2, 2) + field, jnp.float32),
            pltpu.VMEM((3, 2) + field, jnp.float32),
            pltpu.VMEM((LEVELS, 2, own, TILES * LANES), jnp.float32),
            dma((4, TILES)), dma((4, 2)), dma((2, 4)), dma((2, 4)), dma((LEVELS,)), dma((LEVELS,)),
        ],
        compiler_params=pltpu.CompilerParams(
            collective_id=0, has_side_effects=True, vmem_limit_bytes=48 * 1024 * 1024),
        name="window",
    )(u_init, v_init, feed_rate, kill_rate)


def solution(mesh):
    return jax.shard_map(
        body,
        mesh=mesh,
        in_specs=(P("space", None),) * 4,
        out_specs=P("level", None, "space", None),
        check_vma=False,
    )
```

```python
import jax
import jax.numpy as jnp
from jax import lax
from jax.experimental import pallas as pl
from jax.experimental.pallas import tpu as pltpu
from jax.sharding import PartitionSpec as P

STEPS = 4
LEVELS = 4
LANES = 128
TILES = 4
RING = TILES + 1
OFF = 48
REACH = 42
CHUNK = 16
RUN = 4
MESH = pl.DeviceIdType.MESH

FULL = [[42, 39, 36, 15], [32, 29, 26, 11], [22, 19, 16, 7], [12, 9, 6, 3]]
KNOWN = [[10 * level + 3 * step + 6 for step in range(STEPS)] for level in range(LEVELS)]


def room(radius):
    at = (radius + 16) // 8 * 8
    return at, (at + 32 + radius + 16) // 8 * 8


class Field:
    def __init__(self, ref, at):
        self.ref, self.at = ref, at

    def load(self, field, row, rows):
        return self.ref[field, :, pl.ds(row + self.at, rows), :]

    def store(self, field, row, rows, value):
        self.ref[field, :, pl.ds(row + self.at, rows), :] = value

    def around(self, field, row, rows):
        mid = self.load(field, row, rows)
        left = jnp.concatenate([pltpu.roll(mid[RING - 1:], 1, 2), mid[:RING - 1]], 0)
        right = jnp.concatenate([mid[1:], pltpu.roll(mid[:1], LANES - 1, 2)], 0)
        vertical = self.load(field, row - 1, rows) + self.load(field, row + 1, rows)
        return mid, (left + right) + vertical


def over_rows(spans, chunk, body):
    for low, high, upward in spans:
        count = (high - low + 7) // 8 * 8
        if count <= 0:
            continue
        low = high - count if upward else low
        rest = count % chunk
        if rest:
            body(low, rest)

        def step(i, carry, low=low + rest):
            body(low + i * chunk, chunk)
            return carry

        if count // chunk:
            lax.fori_loop(0, count // chunk, step, 0, unroll=True)


def kernel(own, u_hbm, v_hbm, f_hbm, k_hbm, out, inp, nat, turn, fin, turn_out, *rest):
    fields, (load_sem, send_sem, recv_sem, put_sem, got_sem, ready) = list(rest[:-6]), rest[-6:]
    level = lax.axis_index("level")
    space = lax.axis_index("space")
    blocks = lax.axis_size("space")
    cols = TILES * LANES
    after, before = lax.rem(space + 1, blocks), lax.rem(space + blocks - 1, blocks)

    barrier = pltpu.get_barrier_semaphore()
    pl.semaphore_signal(barrier, inc=1, device_id={"space": before}, device_id_type=MESH)
    for step in range(1, LEVELS):
        pl.semaphore_signal(
            barrier, inc=1, device_id={"level": lax.rem(level + step, LEVELS)}, device_id_type=MESH
        )

    starts = [level * cols + tile * LANES for tile in range(TILES)]
    starts.append(lax.rem(level + LEVELS - 1, LEVELS) * cols + cols - LANES)
    starts.append(lax.rem(level + 1, LEVELS) * cols)
    loads = []
    for tile, col in enumerate(starts):
        for at, field in enumerate((u_hbm, v_hbm, f_hbm, k_hbm)):
            loads.append(pltpu.make_async_copy(
                field.at[:, pl.ds(pl.multiple_of(col, LANES), LANES)],
                nat.at[tile, pl.ds(at * own, own), :], load_sem.at[tile, at]))
    for copy in loads:
        copy.start()
    pl.semaphore_wait(barrier, LEVELS)
    pl.semaphore_signal(ready, inc=1, device_id={"space": after}, device_id_type=MESH)
    for copy in loads:
        copy.wait()
    half = lax.broadcasted_iota(jnp.int32, (4 * own, LANES), 1) < LANES // 2
    for tile in range(RING):
        value = nat[tile] if tile < TILES else jnp.where(half, nat[TILES + 1], nat[TILES])
        turn[pl.ds(tile * LANES, LANES), :] = value.T
    for strip in range(RING):
        value = turn[pl.ds(strip, LANES, RING), :].T
        for at in range(3):
            inp[at, strip, pl.ds(OFF, own), :] = value[at * own:(at + 1) * own]
        inp[3, strip, pl.ds(OFF, own), :] = value[2 * own:3 * own] + value[3 * own:]

    far = REACH - own

    def move(at, row, row_there, rows, peer):
        return pltpu.make_async_remote_copy(
            inp.at[:, :, pl.ds(OFF + row, rows), :],
            inp.at[:, :, pl.ds(OFF + row_there, rows), :],
            send_sem.at[at], recv_sem.at[at],
            device_id={"space": peer}, device_id_type=MESH)

    down = [
        move(0, own - far, -far, far, after),
        move(1, 0, -own, own - far, after),
        move(2, -far, -own - far, far, after),
    ]
    up = [
        move(3, 0, own, far, before),
        move(4, far, own + far, own - far, before),
        move(5, own, 2 * own, far, before),
    ]
    down[0].start()
    down[1].start()
    pl.semaphore_wait(ready, 1)
    up[0].start()
    up[1].start()
    down[0].wait_recv()
    down[2].start()
    up[0].wait_recv()
    up[2].start()

    start = Field(inp, OFF)
    rates = Field(inp, OFF)

    def take(radius):
        at, _ = room(radius)
        return Field(fields.pop(0), at)

    first = [take(FULL[1][0]) for _ in range(2)]
    partials = [None] + [take(radii[0]) for radii in FULL[1:]]
    plan = []
    for radii in FULL:
        plan.append([{
            "force": take(radius) if radii is not FULL[0] else None,
            "work": [take(radius - at) for at in range(3)],
            "node": take(radius - 3)} for radius in radii])

    def react(u, v, feed, both):
        cubic = u * v * v
        return feed * (1.0 - u) - cubic, cubic - both * v

    def laps(node, row, rows):
        u, near_u = node.around(0, row, rows)
        v, near_v = node.around(1, row, rows)
        return (u, v), (near_u - 4.0 * u, 0.5 * near_v - 2.0 * v)

    def first_forcing(row, rows):
        feed, both = rates.load(2, row, rows), rates.load(3, row, rows)
        state, lap = laps(start, row, rows)
        rea = react(*state, feed, both)
        for field in range(2):
            total = lap[field] + rea[field]
            first[0].store(field, row, rows, (9.0 / 24.0) * total - rea[field])
            first[1].store(field, row, rows, (1.0 / 24.0) * total)

    def forcing(level_num, row, rows):
        feed, both = rates.load(2, row, rows), rates.load(3, row, rows)
        lap_of, rea_of = [], []
        for at in range(STEPS - 1):
            state, lap = laps(plan[level_num - 1][at]["node"], row, rows)
            lap_of.append(lap)
            rea_of.append(react(*state, feed, both))
        force = [step["force"] for step in plan[level_num]]
        for field in range(2):
            lap = [None] + [value[field] for value in lap_of]
            rea = [None] + [value[field] for value in rea_of]
            full = [None] + [a + b for a, b in zip(lap[1:], rea[1:])]
            nine = first[0].load(field, row, rows)
            one = first[1].load(field, row, rows)
            third = (1.0 / 24.0) * full[3]
            second = (5.0 / 24.0) * full[2]
            force[0].store(field, row, rows, (
                (nine - lap[1]) + (19.0 / 24.0) * full[1] - second + third))
            force[1].store(field, row, rows, (
                (13.0 / 24.0) * (full[1] + full[2]) - (one + third) - (lap[2] + rea[1])))
            force[2].store(field, row, rows, (
                (one - (lap[3] + rea[2])) - (5.0 / 24.0) * full[1]
                + (19.0 / 24.0) * full[2] + (9.0 / 24.0) * full[3]))
            partials[level_num].store(field, row, rows, (
                (1.0 / 24.0) * full[1] - second + (19.0 / 24.0) * full[3] - rea[3]))

    def finish(level_num, row, rows):
        feed, both = rates.load(2, row, rows), rates.load(3, row, rows)
        state, lap = laps(plan[level_num - 1][STEPS - 1]["node"], row, rows)
        rea = react(*state, feed, both)
        for field in range(2):
            plan[level_num][STEPS - 1]["force"].store(field, row, rows, (
                partials[level_num].load(field, row, rows)
                + ((9.0 / 24.0) * rea[field] - (15.0 / 24.0) * lap[field])))

    def source(state, force, dest, row, rows):
        feed, both = rates.load(2, row, rows), rates.load(3, row, rows)
        u, v = state.load(0, row, rows), state.load(1, row, rows)
        rea_u, rea_v = react(u, v, feed, both)
        u = u + rea_u
        v = v + rea_v
        if force is not None:
            u = u + force.load(0, row, rows)
            v = v + force.load(1, row, rows)
        dest.store(0, row, rows, 0.2 * u)
        dest.store(1, row, rows, (1.0 / 3.0) * v)

    def sweep(old, base, new, scales, row, rows):
        for field, scale in enumerate(scales):
            _, total = old.around(field, row, rows)
            if scale != 1.0:
                total = scale * total
            new.store(field, row, rows, base.load(field, row, rows) + total)

    def spans(flip, second, full, known):
        low, high = (-full, min(known, own + full)) if second else (known, own + full)
        if flip:
            low, high = own - high, own - low
        return [(low, high, not flip)]

    def run_level(flip, second, level_num):
        steps = plan[level_num]
        extents = list(zip(FULL[level_num], KNOWN[level_num]))
        if level_num == 1:
            over_rows(spans(flip, second, *extents[0]), 8, first_forcing)
        if level_num:
            over_rows(spans(flip, second, *extents[0]), 8, lambda row, rows: forcing(level_num, row, rows))
            over_rows(spans(flip, second, *extents[3]), 8, lambda row, rows: finish(level_num, row, rows))
        for step_num, step in enumerate(steps):
            state = start if step_num == 0 else steps[step_num - 1]["node"]
            work, (full, known) = step["work"], extents[step_num]
            over_rows(spans(flip, second, full, known), CHUNK,
                      lambda row, rows: source(state, step["force"], work[0], row, rows))
            for sweep_num in range(3):
                new = work[sweep_num + 1] if sweep_num < 2 else step["node"]
                scales = (0.2, 1.0 / 6.0) if sweep_num else (1.0, 0.5)
                over_rows(spans(flip, second, full - sweep_num - 1, known + sweep_num + 1), CHUNK,
                          lambda row, rows: sweep(work[sweep_num], work[0], new, scales, row, rows))

    def handles(level_num):
        place = out.at[0, :, :, pl.ds(pl.multiple_of(level * cols, LANES), cols)]
        mine = pltpu.make_async_copy(fin.at[level_num], place, put_sem.at[level_num])
        theirs = pltpu.make_async_remote_copy(
            fin.at[level_num], place, put_sem.at[level_num], got_sem.at[level],
            device_id={"level": level_num}, device_id_type=MESH)
        return mine, theirs

    def put(level_num):
        node = plan[level_num][STEPS - 1]["node"]
        for strip in range(RING):
            pair = [node.ref[field, strip, pl.ds(node.at, own), :] for field in range(2)]
            turn_out[pl.ds(strip, LANES, RING), :] = jnp.concatenate(pair, 0).T
        for tile in range(TILES):
            value = turn_out[pl.ds(tile * LANES, LANES), :].T
            for field in range(2):
                fin[level_num, field, :, pl.ds(tile * LANES, LANES)] = (
                    value[field * own:(field + 1) * own])
        mine, theirs = handles(level_num)

        @pl.when(level == level_num)
        def _():
            mine.start()

        @pl.when(level != level_num)
        def _():
            theirs.start()

    def window(flip):
        for second in (False, True):
            for copy in down[1:] if second != flip else up[1:]:
                copy.wait_recv()
            for level_num in range(LEVELS):
                run_level(flip, second, level_num)
                if second:
                    put(level_num)

    first_of_run = lax.rem(space, RUN) == 0

    @pl.when(first_of_run)
    def _():
        window(False)

    @pl.when(jnp.logical_not(first_of_run))
    def _():
        window(True)

    for copy in down + up:
        copy.wait_send()
    for level_num in range(LEVELS):
        mine, theirs = handles(level_num)

        @pl.when(level == level_num)
        def _():
            mine.wait()

        @pl.when(level != level_num)
        def _():
            theirs.wait_send()

    for step in range(1, LEVELS):
        source_level = lax.rem(level + step, LEVELS)
        place = out.at[0, :, :, pl.ds(pl.multiple_of(source_level * cols, LANES), cols)]
        pltpu.make_async_remote_copy(
            fin.at[0], place, put_sem.at[0], got_sem.at[source_level],
            device_id={"level": source_level}, device_id_type=MESH).wait_recv()


def body(u_init, v_init, feed_rate, kill_rate):
    own, width = u_init.shape
    dma = pltpu.SemaphoreType.DMA

    def pair(radius):
        return pltpu.VMEM((2, RING, room(radius)[1], LANES), jnp.float32)

    fields = [pair(FULL[1][0])] * 2 + [pair(radii[0]) for radii in FULL[1:]]
    for radii in FULL:
        for radius in radii:
            if radii is not FULL[0]:
                fields.append(pair(radius))
            fields += [pair(radius - at) for at in range(4)]
    return pl.pallas_call(
        lambda *refs: kernel(own, *refs),
        out_shape=pltpu.VMEM((1, 2, own, width), jnp.float32),
        in_specs=[pl.BlockSpec(memory_space=pltpu.HBM)] * 4,
        out_specs=pl.BlockSpec(memory_space=pl.ANY),
        scratch_shapes=[
            pltpu.VMEM((4, RING, OFF + own + OFF + 8, LANES), jnp.float32),
            pltpu.VMEM((TILES + 2, 4 * own, LANES), jnp.float32),
            pltpu.VMEM((RING * LANES, 4 * own), jnp.float32),
            pltpu.VMEM((LEVELS, 2, own, TILES * LANES), jnp.float32),
            pltpu.VMEM((RING * LANES, 2 * own), jnp.float32),
        ] + fields + [
            dma((TILES + 2, 4)), dma((6,)), dma((6,)), dma((LEVELS,)), dma((LEVELS,)),
            pltpu.SemaphoreType.REGULAR,
        ],
        compiler_params=pltpu.CompilerParams(
            collective_id=0, has_side_effects=True, vmem_limit_bytes=48 * 1024 * 1024),
        name="window",
    )(*[pltpu.with_memory_space_constraint(x, pltpu.HBM) for x in (u_init, v_init, feed_rate, kill_rate)])


def solution(mesh):
    return jax.shard_map(
        body,
        mesh=mesh,
        in_specs=(P("space", None),) * 4,
        out_specs=P("level", None, "space", None),
        check_vma=False,
    )
```

```python
import jax
import jax.numpy as jnp
from jax import lax
from jax.experimental import pallas as pl
from jax.experimental.pallas import tpu as pltpu
from jax.sharding import PartitionSpec as P

STEPS = 4
LEVELS = 4
LANES = 128
TILES = 4
RING = TILES + 1
OFF = 48
REACH = 42
REACH_NEAR = 26
CHUNK = 16
RUN = 4
MESH = pl.DeviceIdType.MESH

FULL = [[42, 39, 36, 15], [32, 29, 26, 11], [22, 19, 16, 7], [12, 9, 6, 3]]
NEAR = [[26, 23, 20, 15], [16, 13, 10, 7], [6, 3, 0, -3], [-4, -7, -10, -13]]
KNOWN = [[10 * level + 3 * step + 6 for step in range(STEPS)] for level in range(LEVELS)]


def room(radius):
    at = (radius + 16) // 8 * 8
    return at, (at + 32 + radius + 16) // 8 * 8


class Field:
    def __init__(self, ref, at, side=0):
        self.ref, self.at, self.side = ref, at, side

    def load(self, field, row, rows, side=0):
        strips = pl.ds(self.side - side, RING + 2 * side)
        return self.ref[field, strips, pl.ds(row + self.at, rows), :]

    def store(self, field, row, rows, value):
        if self.side > (value.shape[0] - RING) // 2:
            value = jnp.concatenate([
                pltpu.roll(value[RING - self.side:], 1, 2), value,
                pltpu.roll(value[:self.side], LANES - 1, 2)], 0)
        self.ref[field, :, pl.ds(row + self.at, rows), :] = value

    def around(self, field, row, rows, side=0):
        if self.side > side:
            wide = self.load(field, row, rows, side + 1)
            mid, left, right = wide[1:-1], wide[:-2], wide[2:]
        else:
            mid = self.load(field, row, rows)
            left = jnp.concatenate([pltpu.roll(mid[RING - 1:], 1, 2), mid[:RING - 1]], 0)
            right = jnp.concatenate([mid[1:], pltpu.roll(mid[:1], LANES - 1, 2)], 0)
        vertical = self.load(field, row - 1, rows, side) + self.load(field, row + 1, rows, side)
        return mid, (left + right) + vertical


def over_rows(spans, chunk, body):
    for low, high, upward in spans:
        count = (high - low + 7) // 8 * 8
        if count <= 0:
            continue
        low = high - count if upward else low
        rest = count % chunk
        if rest:
            body(low, rest)

        def step(i, carry, low=low + rest):
            body(low + i * chunk, chunk)
            return carry

        if count // chunk:
            lax.fori_loop(0, count // chunk, step, 0, unroll=True)


def kernel(own, u_hbm, v_hbm, f_hbm, k_hbm, out, inp, nat, turn, fin, turn_out, *rest):
    fields, (load_sem, send_sem, recv_sem, put_sem, got_sem, ready) = list(rest[:-6]), rest[-6:]
    level = lax.axis_index("level")
    space = lax.axis_index("space")
    blocks = lax.axis_size("space")
    cols = TILES * LANES
    after, before = lax.rem(space + 1, blocks), lax.rem(space + blocks - 1, blocks)

    barrier = pltpu.get_barrier_semaphore()
    pl.semaphore_signal(barrier, inc=1, device_id={"space": before}, device_id_type=MESH)
    for step in range(1, LEVELS):
        pl.semaphore_signal(
            barrier, inc=1, device_id={"level": lax.rem(level + step, LEVELS)}, device_id_type=MESH
        )

    starts = [level * cols + tile * LANES for tile in range(TILES)]
    starts.append(lax.rem(level + LEVELS - 1, LEVELS) * cols + cols - LANES)
    starts.append(lax.rem(level + 1, LEVELS) * cols)
    loads = []
    for tile, col in enumerate(starts):
        for at, field in enumerate((u_hbm, v_hbm, f_hbm, k_hbm)):
            loads.append(pltpu.make_async_copy(
                field.at[:, pl.ds(pl.multiple_of(col, LANES), LANES)],
                nat.at[tile, pl.ds(at * own, own), :], load_sem.at[tile, at]))
    for copy in loads:
        copy.start()
    pl.semaphore_wait(barrier, LEVELS)
    pl.semaphore_signal(ready, inc=1, device_id={"space": after}, device_id_type=MESH)
    for copy in loads:
        copy.wait()
    half = lax.broadcasted_iota(jnp.int32, (4 * own, LANES), 1) < LANES // 2
    for tile in range(RING):
        value = nat[tile] if tile < TILES else jnp.where(half, nat[TILES + 1], nat[TILES])
        turn[pl.ds(tile * LANES, LANES), :] = value.T
    for strip in range(RING):
        value = turn[pl.ds(strip, LANES, RING), :].T
        for at in range(3):
            inp[at, strip, pl.ds(OFF, own), :] = value[at * own:(at + 1) * own]
        inp[3, strip, pl.ds(OFF, own), :] = value[2 * own:3 * own] + value[3 * own:]

    far = REACH - own

    def move(at, row, row_there, rows, peer):
        return pltpu.make_async_remote_copy(
            inp.at[:, :, pl.ds(OFF + row, rows), :],
            inp.at[:, :, pl.ds(OFF + row_there, rows), :],
            send_sem.at[at], recv_sem.at[at],
            device_id={"space": peer}, device_id_type=MESH)

    down = [
        move(0, own - far, -far, far, after),
        move(1, own - REACH_NEAR, -REACH_NEAR, REACH_NEAR - far, after),
        move(2, 0, -own, own - REACH_NEAR, after),
        move(3, -far, -own - far, far, after),
    ]
    up = [
        move(4, 0, own, far, before),
        move(5, far, own + far, REACH_NEAR - far, before),
        move(6, REACH_NEAR, own + REACH_NEAR, own - REACH_NEAR, before),
        move(7, own, 2 * own, far, before),
    ]
    for copy in down[:3]:
        copy.start()
    pl.semaphore_wait(ready, 1)
    for copy in up[:3]:
        copy.start()
    down[0].wait_recv()
    down[3].start()
    up[0].wait_recv()
    up[3].start()

    start = Field(inp, OFF)
    rates = Field(inp, OFF)

    def take(radius, side=0):
        at, _ = room(radius)
        return Field(fields.pop(0), at, side)

    first = [take(FULL[1][0]) for _ in range(2)]
    partials = [None] + [take(radii[0]) for radii in FULL[1:]]
    plan = []
    for radii in FULL:
        plan.append([{
            "force": take(radius) if radii is not FULL[0] else None,
            "work": [take(radius - at, 2 - at) for at in range(3)],
            "node": take(radius - 3)} for radius in radii])

    def react(u, v, feed, both):
        cubic = u * v * v
        return feed * (1.0 - u) - cubic, cubic - both * v

    def laps(node, row, rows):
        u, near_u = node.around(0, row, rows)
        v, near_v = node.around(1, row, rows)
        return (u, v), (near_u - 4.0 * u, 0.5 * near_v - 2.0 * v)

    def first_forcing(row, rows):
        feed, both = rates.load(2, row, rows), rates.load(3, row, rows)
        state, lap = laps(start, row, rows)
        rea = react(*state, feed, both)
        for field in range(2):
            total = lap[field] + rea[field]
            first[0].store(field, row, rows, (9.0 / 24.0) * total - rea[field])
            first[1].store(field, row, rows, (1.0 / 24.0) * total)

    def forcing(level_num, row, rows):
        feed, both = rates.load(2, row, rows), rates.load(3, row, rows)
        lap_of, rea_of = [], []
        for at in range(STEPS - 1):
            state, lap = laps(plan[level_num - 1][at]["node"], row, rows)
            lap_of.append(lap)
            rea_of.append(react(*state, feed, both))
        force = [step["force"] for step in plan[level_num]]
        for field in range(2):
            lap = [None] + [value[field] for value in lap_of]
            rea = [None] + [value[field] for value in rea_of]
            full = [None] + [a + b for a, b in zip(lap[1:], rea[1:])]
            nine = first[0].load(field, row, rows)
            one = first[1].load(field, row, rows)
            third = (1.0 / 24.0) * full[3]
            second = (5.0 / 24.0) * full[2]
            force[0].store(field, row, rows, (
                (nine - lap[1]) + (19.0 / 24.0) * full[1] - second + third))
            force[1].store(field, row, rows, (
                (13.0 / 24.0) * (full[1] + full[2]) - (one + third) - (lap[2] + rea[1])))
            force[2].store(field, row, rows, (
                (one - (lap[3] + rea[2])) - (5.0 / 24.0) * full[1]
                + (19.0 / 24.0) * full[2] + (9.0 / 24.0) * full[3]))
            partials[level_num].store(field, row, rows, (
                (1.0 / 24.0) * full[1] - second + (19.0 / 24.0) * full[3] - rea[3]))

    def finish(level_num, row, rows):
        feed, both = rates.load(2, row, rows), rates.load(3, row, rows)
        state, lap = laps(plan[level_num - 1][STEPS - 1]["node"], row, rows)
        rea = react(*state, feed, both)
        for field in range(2):
            plan[level_num][STEPS - 1]["force"].store(field, row, rows, (
                partials[level_num].load(field, row, rows)
                + ((9.0 / 24.0) * rea[field] - (15.0 / 24.0) * lap[field])))

    def source(state, force, dest, row, rows):
        feed, both = rates.load(2, row, rows), rates.load(3, row, rows)
        u, v = state.load(0, row, rows), state.load(1, row, rows)
        rea_u, rea_v = react(u, v, feed, both)
        u = u + rea_u
        v = v + rea_v
        if force is not None:
            u = u + force.load(0, row, rows)
            v = v + force.load(1, row, rows)
        dest.store(0, row, rows, 0.2 * u)
        dest.store(1, row, rows, (1.0 / 3.0) * v)

    def sweep(old, base, new, scales, row, rows):
        for field, scale in enumerate(scales):
            _, total = old.around(field, row, rows, new.side)
            if scale != 1.0:
                total = scale * total
            new.store(field, row, rows, base.load(field, row, rows, new.side) + total)

    def spans(flip, stage, full, near, known):
        known = min(known, own + full)
        low, high = {"below": (known, own + full), "near": (-near, known), "far": (-full, -near)}[stage]
        if flip:
            low, high = own - high, own - low
        return [(low, high, not flip)]

    def run_level(flip, stage, level_num):
        steps = plan[level_num]
        extents = list(zip(FULL[level_num], NEAR[level_num], KNOWN[level_num]))
        if level_num == 1:
            over_rows(spans(flip, stage, *extents[0]), 8, first_forcing)
        if level_num:
            over_rows(spans(flip, stage, *extents[0]), 8, lambda row, rows: forcing(level_num, row, rows))
            over_rows(spans(flip, stage, *extents[3]), 8, lambda row, rows: finish(level_num, row, rows))
        for step_num, step in enumerate(steps):
            state = start if step_num == 0 else steps[step_num - 1]["node"]
            work, (full, near, known) = step["work"], extents[step_num]
            over_rows(spans(flip, stage, full, near, known), CHUNK,
                      lambda row, rows: source(state, step["force"], work[0], row, rows))
            for sweep_num in range(3):
                new = work[sweep_num + 1] if sweep_num < 2 else step["node"]
                scales = (0.2, 1.0 / 6.0) if sweep_num else (1.0, 0.5)
                over_rows(spans(
                    flip, stage, full - sweep_num - 1, near - sweep_num - 1, known + sweep_num + 1), CHUNK,
                          lambda row, rows: sweep(work[sweep_num], work[0], new, scales, row, rows))

    part = own // 2

    def handles(level_num, half):
        rows = pl.ds(half * part, part)
        place = out.at[0, :, rows, pl.ds(pl.multiple_of(level * cols, LANES), cols)]
        mine = pltpu.make_async_copy(fin.at[level_num, :, rows], place, put_sem.at[level_num, half])
        theirs = pltpu.make_async_remote_copy(
            fin.at[level_num, :, rows], place, put_sem.at[level_num, half], got_sem.at[level, half],
            device_id={"level": level_num}, device_id_type=MESH)
        return mine, theirs

    def put(level_num, halves):
        node = plan[level_num][STEPS - 1]["node"]
        first_row, count = halves[0] * part, len(halves) * part
        lanes = pl.ds(0, 2 * count)
        for strip in range(RING):
            pair = [node.ref[field, strip, pl.ds(node.at + first_row, count), :] for field in range(2)]
            turn_out[pl.ds(strip, LANES, RING), lanes] = jnp.concatenate(pair, 0).T
        for tile in range(TILES):
            value = turn_out[pl.ds(tile * LANES, LANES), lanes].T
            for field in range(2):
                fin[level_num, field, pl.ds(first_row, count), pl.ds(tile * LANES, LANES)] = (
                    value[field * count:(field + 1) * count])

        @pl.when(level == level_num)
        def _():
            for half in halves:
                handles(level_num, half)[0].start()

        @pl.when(level != level_num)
        def _():
            for half in halves:
                handles(level_num, half)[1].start()

    def window(flip):
        early, late = (down, up) if flip else (up, down)
        known_first, known_last = (0, 1) if flip else (1, 0)
        for copy in early[1:]:
            copy.wait_recv()
        for level_num in range(LEVELS):
            run_level(flip, "below", level_num)
        late[1].wait_recv()
        for level_num in range(LEVELS):
            run_level(flip, "near", level_num)
            put(level_num, (0, 1) if level_num < 2 else (known_first,))
        late[2].wait_recv()
        late[3].wait_recv()
        for level_num in range(LEVELS):
            run_level(flip, "far", level_num)
            if level_num >= 2:
                put(level_num, (known_last,))

    first_of_run = lax.rem(space, RUN) < RUN // 2

    @pl.when(first_of_run)
    def _():
        window(False)

    @pl.when(jnp.logical_not(first_of_run))
    def _():
        window(True)

    for copy in down + up:
        copy.wait_send()
    for level_num in range(LEVELS):
        @pl.when(level == level_num)
        def _():
            for half in range(2):
                handles(level_num, half)[0].wait()

        @pl.when(level != level_num)
        def _():
            for half in range(2):
                handles(level_num, half)[1].wait_send()

    for step in range(1, LEVELS):
        source_level = lax.rem(level + step, LEVELS)
        for half in range(2):
            rows = pl.ds(half * part, part)
            place = out.at[0, :, rows, pl.ds(pl.multiple_of(source_level * cols, LANES), cols)]
            pltpu.make_async_remote_copy(
                fin.at[0, :, rows], place, put_sem.at[0, half], got_sem.at[source_level, half],
                device_id={"level": source_level}, device_id_type=MESH).wait_recv()


def body(u_init, v_init, feed_rate, kill_rate):
    own, width = u_init.shape
    dma = pltpu.SemaphoreType.DMA

    def pair(radius, side=0):
        return pltpu.VMEM((2, RING + 2 * side, room(radius)[1], LANES), jnp.float32)

    fields = [pair(FULL[1][0])] * 2 + [pair(radii[0]) for radii in FULL[1:]]
    for radii in FULL:
        for radius in radii:
            if radii is not FULL[0]:
                fields.append(pair(radius))
            fields += [pair(radius - at, max(2 - at, 0)) for at in range(4)]
    return pl.pallas_call(
        lambda *refs: kernel(own, *refs),
        out_shape=pltpu.VMEM((1, 2, own, width), jnp.float32),
        in_specs=[pl.BlockSpec(memory_space=pltpu.HBM)] * 4,
        out_specs=pl.BlockSpec(memory_space=pl.ANY),
        scratch_shapes=[
            pltpu.VMEM((4, RING, OFF + own + OFF + 8, LANES), jnp.float32),
            pltpu.VMEM((TILES + 2, 4 * own, LANES), jnp.float32),
            pltpu.VMEM((RING * LANES, 4 * own), jnp.float32),
            pltpu.VMEM((LEVELS, 2, own, TILES * LANES), jnp.float32),
            pltpu.VMEM((RING * LANES, 2 * own), jnp.float32),
        ] + fields + [
            dma((TILES + 2, 4)), dma((8,)), dma((8,)), dma((LEVELS, 2)), dma((LEVELS, 2)),
            pltpu.SemaphoreType.REGULAR,
        ],
        compiler_params=pltpu.CompilerParams(
            collective_id=0, has_side_effects=True, vmem_limit_bytes=56 * 1024 * 1024),
        name="window",
    )(*[pltpu.with_memory_space_constraint(x, pltpu.HBM) for x in (u_init, v_init, feed_rate, kill_rate)])


def solution(mesh):
    return jax.shard_map(
        body,
        mesh=mesh,
        in_specs=(P("space", None),) * 4,
        out_specs=P("level", None, "space", None),
        check_vma=False,
    )
```

```python
import jax
import jax.numpy as jnp
from jax import lax
from jax.experimental import pallas as pl
from jax.experimental.pallas import tpu as pltpu
from jax.sharding import PartitionSpec as P

STEPS = 4
LEVELS = 4
LANES = 128
TILES = 4
RING = TILES + 1
OFF = 48
REACH = 42
REACH_NEAR = 26
CHUNK = 16
PARTS = 4
RUN = 4
MESH = pl.DeviceIdType.MESH

FULL = [[42, 39, 36, 15], [32, 29, 26, 11], [22, 19, 16, 7], [12, 9, 6, 3]]
NEAR = [[26, 23, 20, 15], [16, 13, 10, 7], [6, 3, 0, -3], [-4, -7, -10, -13]]
KNOWN = [[10 * level + 3 * step + 6 for step in range(STEPS)] for level in range(LEVELS)]


def room(radius):
    at = (radius + 16) // 8 * 8
    return at, (at + 32 + radius + 16) // 8 * 8


class Field:
    def __init__(self, ref, at, side=0):
        self.ref, self.at, self.side = ref, at, side

    def load(self, field, row, rows, side=0):
        strips = pl.ds(self.side - side, RING + 2 * side)
        return self.ref[field, strips, pl.ds(row + self.at, rows), :]

    def store(self, field, row, rows, value):
        if self.side > (value.shape[0] - RING) // 2:
            value = jnp.concatenate([
                pltpu.roll(value[RING - self.side:], 1, 2), value,
                pltpu.roll(value[:self.side], LANES - 1, 2)], 0)
        self.ref[field, :, pl.ds(row + self.at, rows), :] = value

    def around(self, field, row, rows, side=0):
        if self.side > side:
            wide = self.load(field, row, rows, side + 1)
            mid, left, right = wide[1:-1], wide[:-2], wide[2:]
        else:
            mid = self.load(field, row, rows)
            left = jnp.concatenate([pltpu.roll(mid[RING - 1:], 1, 2), mid[:RING - 1]], 0)
            right = jnp.concatenate([mid[1:], pltpu.roll(mid[:1], LANES - 1, 2)], 0)
        vertical = self.load(field, row - 1, rows, side) + self.load(field, row + 1, rows, side)
        return mid, (left + right) + vertical


def over_rows(spans, chunk, body):
    for low, high, upward in spans:
        count = (high - low + 7) // 8 * 8
        if count <= 0:
            continue
        low = high - count if upward else low
        rest = count % chunk
        if rest:
            body(low, rest)

        def step(i, carry, low=low + rest):
            body(low + i * chunk, chunk)
            return carry

        if count // chunk:
            lax.fori_loop(0, count // chunk, step, 0, unroll=True)


def kernel(own, u_hbm, v_hbm, f_hbm, k_hbm, out, inp, nat, turn, fin, turn_out, *rest):
    fields, (load_sem, send_sem, recv_sem, put_sem, got_sem, ready) = list(rest[:-6]), rest[-6:]
    level = lax.axis_index("level")
    space = lax.axis_index("space")
    blocks = lax.axis_size("space")
    cols = TILES * LANES
    after, before = lax.rem(space + 1, blocks), lax.rem(space + blocks - 1, blocks)

    barrier = pltpu.get_barrier_semaphore()
    pl.semaphore_signal(barrier, inc=1, device_id={"space": before}, device_id_type=MESH)
    for step in range(1, LEVELS):
        pl.semaphore_signal(
            barrier, inc=1, device_id={"level": lax.rem(level + step, LEVELS)}, device_id_type=MESH
        )

    starts = [level * cols + tile * LANES for tile in range(TILES)]
    starts.append(lax.rem(level + LEVELS - 1, LEVELS) * cols + cols - LANES)
    starts.append(lax.rem(level + 1, LEVELS) * cols)
    loads = []
    for tile, col in enumerate(starts):
        for at, field in enumerate((u_hbm, v_hbm, f_hbm, k_hbm)):
            loads.append(pltpu.make_async_copy(
                field.at[:, pl.ds(pl.multiple_of(col, LANES), LANES)],
                nat.at[tile, pl.ds(at * own, own), :], load_sem.at[tile, at]))
    for copy in loads:
        copy.start()
    pl.semaphore_wait(barrier, LEVELS)
    pl.semaphore_signal(ready, inc=1, device_id={"space": after}, device_id_type=MESH)
    for copy in loads:
        copy.wait()
    half = lax.broadcasted_iota(jnp.int32, (4 * own, LANES), 1) < LANES // 2
    for tile in range(RING):
        value = nat[tile] if tile < TILES else jnp.where(half, nat[TILES + 1], nat[TILES])
        turn[pl.ds(tile * LANES, LANES), :] = value.T
    for strip in range(RING):
        value = turn[pl.ds(strip, LANES, RING), :].T
        for at in range(3):
            inp[at, strip, pl.ds(OFF, own), :] = value[at * own:(at + 1) * own]
        inp[3, strip, pl.ds(OFF, own), :] = value[2 * own:3 * own] + value[3 * own:]

    far = REACH - own

    def move(at, row, row_there, rows, peer):
        return pltpu.make_async_remote_copy(
            inp.at[:, :, pl.ds(OFF + row, rows), :],
            inp.at[:, :, pl.ds(OFF + row_there, rows), :],
            send_sem.at[at], recv_sem.at[at],
            device_id={"space": peer}, device_id_type=MESH)

    down = [
        move(0, own - far, -far, far, after),
        move(1, own - REACH_NEAR, -REACH_NEAR, REACH_NEAR - far, after),
        move(2, 0, -own, own - REACH_NEAR, after),
        move(3, -far, -own - far, far, after),
    ]
    up = [
        move(4, 0, own, far, before),
        move(5, far, own + far, REACH_NEAR - far, before),
        move(6, REACH_NEAR, own + REACH_NEAR, own - REACH_NEAR, before),
        move(7, own, 2 * own, far, before),
    ]
    for copy in down[:3]:
        copy.start()
    pl.semaphore_wait(ready, 1)
    for copy in up[:3]:
        copy.start()

    start = Field(inp, OFF)
    rates = Field(inp, OFF)

    def take(radius, side=0):
        at, _ = room(radius)
        return Field(fields.pop(0), at, side)

    first = [take(FULL[1][0]) for _ in range(2)]
    partials = [None] + [take(radii[0]) for radii in FULL[1:]]
    plan = []
    for radii in FULL:
        plan.append([{
            "force": take(radius) if radii is not FULL[0] else None,
            "work": [take(radius - at, 2 - at) for at in range(3)],
            "node": take(radius - 3)} for radius in radii])

    def react(u, v, feed, both):
        cubic = u * v * v
        return feed * (1.0 - u) - cubic, cubic - both * v

    def laps(node, row, rows):
        u, near_u = node.around(0, row, rows)
        v, near_v = node.around(1, row, rows)
        return (u, v), (near_u - 4.0 * u, 0.5 * near_v - 2.0 * v)

    def first_forcing(row, rows):
        feed, both = rates.load(2, row, rows), rates.load(3, row, rows)
        state, lap = laps(start, row, rows)
        rea = react(*state, feed, both)
        for field in range(2):
            total = lap[field] + rea[field]
            first[0].store(field, row, rows, (9.0 / 24.0) * total - rea[field])
            first[1].store(field, row, rows, (1.0 / 24.0) * total)

    def forcing(level_num, row, rows):
        feed, both = rates.load(2, row, rows), rates.load(3, row, rows)
        lap_of, rea_of = [], []
        for at in range(STEPS - 1):
            state, lap = laps(plan[level_num - 1][at]["node"], row, rows)
            lap_of.append(lap)
            rea_of.append(react(*state, feed, both))
        force = [step["force"] for step in plan[level_num]]
        for field in range(2):
            lap = [None] + [value[field] for value in lap_of]
            rea = [None] + [value[field] for value in rea_of]
            full = [None] + [a + b for a, b in zip(lap[1:], rea[1:])]
            nine = first[0].load(field, row, rows)
            one = first[1].load(field, row, rows)
            third = (1.0 / 24.0) * full[3]
            second = (5.0 / 24.0) * full[2]
            force[0].store(field, row, rows, (
                (nine - lap[1]) + (19.0 / 24.0) * full[1] - second + third))
            force[1].store(field, row, rows, (
                (13.0 / 24.0) * (full[1] + full[2]) - (one + third) - (lap[2] + rea[1])))
            force[2].store(field, row, rows, (
                (one - (lap[3] + rea[2])) - (5.0 / 24.0) * full[1]
                + (19.0 / 24.0) * full[2] + (9.0 / 24.0) * full[3]))
            partials[level_num].store(field, row, rows, (
                (1.0 / 24.0) * full[1] - second + (19.0 / 24.0) * full[3] - rea[3]))

    def finish(level_num, row, rows):
        feed, both = rates.load(2, row, rows), rates.load(3, row, rows)
        state, lap = laps(plan[level_num - 1][STEPS - 1]["node"], row, rows)
        rea = react(*state, feed, both)
        for field in range(2):
            plan[level_num][STEPS - 1]["force"].store(field, row, rows, (
                partials[level_num].load(field, row, rows)
                + ((9.0 / 24.0) * rea[field] - (15.0 / 24.0) * lap[field])))

    def source(state, force, dest, row, rows):
        feed, both = rates.load(2, row, rows), rates.load(3, row, rows)
        u, v = state.load(0, row, rows), state.load(1, row, rows)
        rea_u, rea_v = react(u, v, feed, both)
        u = u + rea_u
        v = v + rea_v
        if force is not None:
            u = u + force.load(0, row, rows)
            v = v + force.load(1, row, rows)
        dest.store(0, row, rows, 0.2 * u)
        dest.store(1, row, rows, (1.0 / 3.0) * v)

    def sweep(old, base, new, scales, row, rows):
        for field, scale in enumerate(scales):
            _, total = old.around(field, row, rows, new.side)
            if scale != 1.0:
                total = scale * total
            new.store(field, row, rows, base.load(field, row, rows, new.side) + total)

    def spans(stage, full, near, known):
        name, flip = stage
        known = min(known, own + full)
        rows = {
            "half": [(known, own + near, True)],
            "below": [(max(known, own + near), own + full, False)],
            "near": [(-near, known, True)],
            "far": [(-full, -near, True)],
        }[name]
        if flip:
            rows = [(own - high, own - low, not upward) for low, high, upward in rows]
        return rows

    def run_level(stage, level_num):
        steps = plan[level_num]
        extents = list(zip(FULL[level_num], NEAR[level_num], KNOWN[level_num]))
        if level_num == 1:
            over_rows(spans(stage, *extents[0]), 8, first_forcing)
        if level_num:
            over_rows(spans(stage, *extents[0]), 8, lambda row, rows: forcing(level_num, row, rows))
            over_rows(spans(stage, *extents[3]), 8, lambda row, rows: finish(level_num, row, rows))
        for step_num, step in enumerate(steps):
            state = start if step_num == 0 else steps[step_num - 1]["node"]
            work, (full, near, known) = step["work"], extents[step_num]
            over_rows(spans(stage, full, near, known), CHUNK,
                      lambda row, rows: source(state, step["force"], work[0], row, rows))
            for sweep_num in range(3):
                new = work[sweep_num + 1] if sweep_num < 2 else step["node"]
                scales = (0.2, 1.0 / 6.0) if sweep_num else (1.0, 0.5)
                over_rows(spans(
                    stage, full - sweep_num - 1, near - sweep_num - 1, known + sweep_num + 1), CHUNK,
                          lambda row, rows: sweep(work[sweep_num], work[0], new, scales, row, rows))

    part = own // PARTS

    def handles(level_num, half):
        rows = pl.ds(half * part, part)
        place = out.at[0, :, rows, pl.ds(pl.multiple_of(level * cols, LANES), cols)]
        mine = pltpu.make_async_copy(fin.at[level_num, :, rows], place, put_sem.at[level_num, half])
        theirs = pltpu.make_async_remote_copy(
            fin.at[level_num, :, rows], place, put_sem.at[level_num, half], got_sem.at[level, half],
            device_id={"level": level_num}, device_id_type=MESH)
        return mine, theirs

    def put(level_num, halves):
        node = plan[level_num][STEPS - 1]["node"]
        count = len(halves) * part
        lanes = pl.ds(0, 2 * count)
        for strip in range(RING):
            pieces = [node.ref[field, strip, pl.ds(node.at + half * part, part), :]
                      for field in range(2) for half in halves]
            turn_out[pl.ds(strip, LANES, RING), lanes] = jnp.concatenate(pieces, 0).T
        for tile in range(TILES):
            value = turn_out[pl.ds(tile * LANES, LANES), lanes].T
            for field in range(2):
                for at, half in enumerate(halves):
                    row = field * count + at * part
                    fin[level_num, field, pl.ds(half * part, part), pl.ds(tile * LANES, LANES)] = (
                        value[row:row + part])

        @pl.when(level == level_num)
        def _():
            for half in halves:
                handles(level_num, half)[0].start()

        @pl.when(level != level_num)
        def _():
            for half in halves:
                handles(level_num, half)[1].start()

    every = tuple(range(PARTS))

    def one_side(flip):
        early, late = (down, up) if flip else (up, down)
        early[0].wait_recv()
        early[3].start()
        early[1].wait_recv()
        for level_num in range(LEVELS):
            run_level(("half", flip), level_num)
        late[0].wait_recv()
        late[3].start()
        for copy in early[2:]:
            copy.wait_recv()
        for level_num in range(LEVELS):
            run_level(("below", flip), level_num)
        late[1].wait_recv()
        for level_num in range(LEVELS):
            run_level(("near", flip), level_num)
            pieces = (every, every, (1, 2, 3), (2, 3))[level_num]
            put(level_num, tuple(sorted(PARTS - 1 - piece for piece in pieces)) if flip else pieces)
        late[2].wait_recv()
        late[3].wait_recv()
        for level_num in range(LEVELS):
            run_level(("far", flip), level_num)
            if level_num >= 2:
                pieces = ((0,), (0, 1))[level_num - 2]
                put(level_num, tuple(sorted(PARTS - 1 - piece for piece in pieces)) if flip else pieces)

    first_half = lax.rem(space, RUN) < RUN // 2
    pl.when(first_half)(lambda: one_side(False))
    pl.when(jnp.logical_not(first_half))(lambda: one_side(True))

    for copy in down + up:
        copy.wait_send()
    for level_num in range(LEVELS):
        @pl.when(level == level_num)
        def _():
            for half in range(PARTS):
                handles(level_num, half)[0].wait()

        @pl.when(level != level_num)
        def _():
            for half in range(PARTS):
                handles(level_num, half)[1].wait_send()

    for step in range(1, LEVELS):
        source_level = lax.rem(level + step, LEVELS)
        for half in range(PARTS):
            rows = pl.ds(half * part, part)
            place = out.at[0, :, rows, pl.ds(pl.multiple_of(source_level * cols, LANES), cols)]
            pltpu.make_async_remote_copy(
                fin.at[0, :, rows], place, put_sem.at[0, half], got_sem.at[source_level, half],
                device_id={"level": source_level}, device_id_type=MESH).wait_recv()


def body(u_init, v_init, feed_rate, kill_rate):
    own, width = u_init.shape
    dma = pltpu.SemaphoreType.DMA

    def pair(radius, side=0):
        return pltpu.VMEM((2, RING + 2 * side, room(radius)[1], LANES), jnp.float32)

    fields = [pair(FULL[1][0])] * 2 + [pair(radii[0]) for radii in FULL[1:]]
    for radii in FULL:
        for radius in radii:
            if radii is not FULL[0]:
                fields.append(pair(radius))
            fields += [pair(radius - at, max(2 - at, 0)) for at in range(4)]
    return pl.pallas_call(
        lambda *refs: kernel(own, *refs),
        out_shape=pltpu.VMEM((1, 2, own, width), jnp.float32),
        in_specs=[pl.BlockSpec(memory_space=pltpu.HBM)] * 4,
        out_specs=pl.BlockSpec(memory_space=pl.ANY),
        scratch_shapes=[
            pltpu.VMEM((4, RING, OFF + own + OFF + 8, LANES), jnp.float32),
            pltpu.VMEM((TILES + 2, 4 * own, LANES), jnp.float32),
            pltpu.VMEM((RING * LANES, 4 * own), jnp.float32),
            pltpu.VMEM((LEVELS, 2, own, TILES * LANES), jnp.float32),
            pltpu.VMEM((RING * LANES, 2 * own), jnp.float32),
        ] + fields + [
            dma((TILES + 2, 4)), dma((8,)), dma((8,)), dma((LEVELS, PARTS)), dma((LEVELS, PARTS)),
            pltpu.SemaphoreType.REGULAR,
        ],
        compiler_params=pltpu.CompilerParams(
            collective_id=0, has_side_effects=True, vmem_limit_bytes=56 * 1024 * 1024),
        name="window",
    )(*[pltpu.with_memory_space_constraint(x, pltpu.HBM) for x in (u_init, v_init, feed_rate, kill_rate)])


def solution(mesh):
    return jax.shard_map(
        body,
        mesh=mesh,
        in_specs=(P("space", None),) * 4,
        out_specs=P("level", None, "space", None),
        check_vma=False,
    )
```
